32 devices in a mesh: gene: 8 (over z, x), cell: 4 (over y, core).
Axes of the slice: x: 2, y: 2, z: 4, core: 2. Of those that a mesh axis runs over, the one named last changes fastest.
Arguments:
- pool_counts: bfloat16 [20480, 16384], P('gene', 'cell'), may hold values from 0 to 6.5
- cell_picks: int32 [7, 4096], P(None, 'cell'), may hold values from 0 to 16383, as said below
- loadings_init: float32 [64, 20480], P(None, 'gene'), may hold values from -0.0390625 to 0.0390625
Outputs:
- scaled_loadings: float32 [64, 20480], P(None, 'gene')
The draws below stay inside these ranges and needn't reach their ends.
Inputs may be any that keep to these rules, and one draw needn't show every extreme that they name: `cell_picks`: column b of every row names a pool cell in [(b // 1024) * 4096, (b // 1024 + 1) * 4096); no cell is named twice in one row.
All inputs are finite; a program needn't handle non-finite values.
Results may differ from the reference program's by a relative error of at most 0.018.
Values may be sent and summed in bfloat16 or wider, within the bound.
A program may use at most 128 MiB of HBM per device.

```python
import math
import jax
import jax.numpy as jnp
from jax import lax

GENES = 20480
COMPS = 64
STEPS = 7
BATCH_DEV = 1024
POOL_DEV = 4096
BATCH = 4096
POOL = 16384


def draw_pool_counts(key, part):
    scale_key, noise_key = jax.random.split(jax.random.fold_in(key, 11))
    genes = jnp.arange(GENES, dtype=jnp.float32)
    rising = 1.0 + 2.0 * genes / max(GENES - 1, 1)
    lowest, highest = (math.log(0.1), math.log(10.0))
    gene_scale = jnp.exp(jax.random.uniform(scale_key, (GENES,), jnp.float32, lowest, highest)) * rising
    noise = jnp.minimum(jax.random.exponential(noise_key, (GENES, POOL), jnp.float32), 12.0)
    return jnp.log1p(gene_scale[:, None] * noise).astype(jnp.bfloat16)


def draw_cell_picks(key, part):
    base = jax.random.fold_in(key, 23)
    rows = []
    for step_index in range(STEPS):
        pieces = []
        for group_index in range(BATCH // BATCH_DEV):
            group_key = jax.random.fold_in(jax.random.fold_in(base, step_index), group_index)
            order = jax.random.permutation(group_key, POOL_DEV).astype(jnp.int32)
            pieces.append(order[:BATCH_DEV] + group_index * POOL_DEV)
        rows.append(jnp.concatenate(pieces))
    return jnp.stack(rows).astype(jnp.int32)


def steps_of(rng, extent, cuts, low, top_value):
    level = 1.0
    for position, shards_of in cuts:
        draws = jax.random.uniform(jax.random.fold_in(jax.random.fold_in(rng, 6), position), (shards_of,), jnp.float32, low / len(cuts), top_value / len(cuts))
        level = level * jnp.repeat(jnp.exp(draws), extent[position] // shards_of).reshape((-1,) + (1,) * (len(extent) - 1 - position))
    return level


def bell_draw(own_key, dims, scale, limit, cuts=(), kind=jnp.bfloat16):
    loudness = steps_of(own_key, dims, cuts, -0.22, 0.18) if cuts else 1.0
    drawn = jax.random.normal(own_key, dims, jnp.float32) * scale * loudness
    return jnp.minimum(jnp.maximum(drawn, -limit), limit).astype(kind)


def setup_inputs(seed: int = 0) -> dict:
    seeds = jax.random.split(jax.random.key(seed), 4)
    return {
        "pool_counts": draw_pool_counts(jax.random.fold_in(seeds[3], 71), 0),
        "cell_picks": draw_cell_picks(jax.random.fold_in(seeds[3], 71), 0),
        "loadings_init": bell_draw(seeds[2], (COMPS, GENES), GENES ** -0.5, 0.0390625, ((1, 8),), jnp.float32),
    }


step_rate = 1.0

def reference(pool_counts, cell_picks, loadings_init):
    loadings = loadings_init
    block_width = GENES // 8
    for step_index in range(STEPS):
        chosen = cell_picks[step_index]
        weights_low = loadings.astype(jnp.bfloat16)
        scores = jnp.zeros((COMPS, BATCH), jnp.float32)
        batch_means = []
        for block_index in range(8):
            lowest = block_index * block_width
            gathered = jnp.take(pool_counts[lowest:lowest + block_width], chosen, axis=1)
            means_part = lax.optimization_barrier(jnp.sum(gathered.astype(jnp.float32), axis=1)) / BATCH
            weight_part = weights_low[:, lowest:lowest + block_width]
            scores = scores + jnp.dot(weight_part.astype(jnp.float32), gathered.astype(jnp.float32), preferred_element_type=jnp.float32)
            shift = jnp.dot(weight_part.astype(jnp.float32), means_part, precision=lax.Precision.HIGHEST)
            scores = scores - shift[:, None]
            batch_means.append(means_part)
        scores_low = scores.astype(jnp.bfloat16)
        row_totals = lax.optimization_barrier(jnp.sum(scores_low.astype(jnp.float32), axis=1))
        updates = []
        for block_index in range(8):
            lowest = block_index * block_width
            gathered = jnp.take(pool_counts[lowest:lowest + block_width], chosen, axis=1)
            raw_update = lax.dot_general(scores_low.astype(jnp.float32), gathered.astype(jnp.float32), (((1,), (1,)), ((), ())), preferred_element_type=jnp.float32)
            updates.append((raw_update - row_totals[:, None] * batch_means[block_index][None, :]) / BATCH)
        update = jnp.concatenate(updates, axis=1)
        stepped = loadings + step_rate * update
        gram_matrix = jnp.dot(stepped, stepped.T, precision=lax.Precision.HIGHEST)
        factor = jnp.linalg.cholesky(gram_matrix)
        loadings = lax.linalg.triangular_solve(factor, stepped, left_side=True, lower=True)
    return loadings * math.sqrt(GENES)
```

```python
import functools
import math

import jax
import jax.numpy as jnp
from jax import lax
from jax.experimental import pallas as pl
from jax.experimental.pallas import tpu as pltpu
from jax.sharding import PartitionSpec as P

STEPS = 7
MESH = pl.DeviceIdType.MESH

step_rate = 1.0


def transposed_product(left, right):
    return lax.dot_general(
        left, right, (((1,), (1,)), ((), ())), preferred_element_type=jnp.float32
    )


def sum_kernel(axis, n, arrays, gather, *refs):
    inputs = refs[:arrays]
    refs = refs[arrays:]
    if gather:
        pool_ref, picks_ref = refs[:2]
        refs = refs[2:]
    outputs = refs[:arrays]
    refs = refs[arrays:]
    if gather:
        tile_ref = refs[0]
        refs = refs[1:]
    landed, reduced, whole = (refs[i * arrays:(i + 1) * arrays] for i in range(3))
    sends, arrivals, sends_back, arrivals_back = refs[3 * arrays:3 * arrays + 4]
    me = lax.axis_index(axis)
    barrier = pltpu.get_barrier_semaphore()
    peers = [lax.rem(me + k, n) for k in range(n)]
    for k in range(1, n):
        pl.semaphore_signal(barrier, inc=1, device_id={axis: peers[k]}, device_id_type=MESH)
    blocks = 0
    if gather:
        held, hot, loaded = refs[3 * arrays + 4:]
        start, block, blocks = gather
        loads = []
        for b in range(blocks):
            load = pltpu.make_async_copy(
                pool_ref.at[pl.ds(start + b * block, block)],
                held.at[pl.ds(b * block, block)],
                loaded.at[b],
            )
            load.start()
            loads.append(load)

    def select_columns(b):
        loads[b].wait()
        rows = pl.ds(b * block, block)
        width = min(512, hot.shape[1])

        def piece(j, carry):
            columns = pl.ds(pl.multiple_of(j * width, width), width)
            tile_ref[rows, columns] = jnp.dot(
                held[rows, :], hot[:, columns], preferred_element_type=jnp.float32
            ).astype(tile_ref.dtype)
            return carry

        lax.fori_loop(0, hot.shape[1] // width, piece, 0)

    pl.semaphore_wait(barrier, n - 1)
    copies = []
    for a in range(arrays):
        for k in range(1, n):
            copy = pltpu.make_async_remote_copy(
                src_ref=inputs[a].at[peers[k]],
                dst_ref=landed[a].at[k - 1],
                send_sem=sends.at[a, k - 1],
                recv_sem=arrivals.at[a, k - 1],
                device_id={axis: peers[k]},
                device_id_type=MESH,
            )
            copy.start()
            copies.append(copy)
    if gather:
        depth = 256

        def mark(i, carry):
            ids = lax.broadcasted_iota(jnp.int32, (depth, hot.shape[1]), 0) + i * depth
            hot[pl.ds(pl.multiple_of(i * depth, depth), depth), :] = jnp.where(
                ids == picks_ref[...], 1.0, 0.0
            ).astype(hot.dtype)
            return carry

        lax.fori_loop(0, hot.shape[0] // depth, mark, 0)
    early = blocks // 2
    for b in range(early):
        select_columns(b)
    for copy in copies:
        copy.wait_recv()
    backs = []
    for a in range(arrays):
        total = inputs[a][me].astype(jnp.float32)
        for k in range(1, n):
            total = total + landed[a][k - 1].astype(jnp.float32)
        reduced[a][...] = total.astype(reduced[a].dtype)
        for k in range(1, n):
            copy = pltpu.make_async_remote_copy(
                src_ref=reduced[a],
                dst_ref=whole[a].at[me],
                send_sem=sends_back.at[a, k - 1],
                recv_sem=arrivals_back.at[a, k - 1],
                device_id={axis: peers[k]},
                device_id_type=MESH,
            )
            copy.start()
            backs.append(copy)
        outputs[a][me] = reduced[a][...]
    for b in range(early, blocks):
        select_columns(b)
    for copy in copies:
        copy.wait_send()
    for copy in backs:
        copy.wait()
    for a in range(arrays):
        for k in range(1, n):
            outputs[a][peers[k]] = whole[a][peers[k]]


def sum_over(axis, n, collective_id, arrays, gather=None):
    cut = [a.reshape(n, a.shape[0] // n, a.shape[1]) for a in arrays]
    count = len(cut)
    vmem = pl.BlockSpec(memory_space=pltpu.VMEM)
    operands, in_specs = list(cut), [vmem] * count
    shapes = [jax.ShapeDtypeStruct(a.shape, a.dtype) for a in cut]
    scratch = [pltpu.VMEM((n - 1,) + a.shape[1:], a.dtype) for a in cut]
    scratch += [pltpu.VMEM(a.shape[1:], a.dtype) for a in cut]
    scratch += [pltpu.VMEM(a.shape, a.dtype) for a in cut]
    scratch += [pltpu.SemaphoreType.DMA((count, n - 1))] * 4
    plan = None
    if gather is not None:
        pool, picks, start, rows = gather
        block = 256 if rows % 256 == 0 else rows
        plan = (start, block, rows // block)
        operands += [pool, picks[None, :]]
        in_specs += [pl.BlockSpec(memory_space=pl.ANY), vmem]
        shapes.append(jax.ShapeDtypeStruct((rows, picks.shape[0]), pool.dtype))
        scratch += [
            pltpu.VMEM((rows, pool.shape[1]), pool.dtype),
            pltpu.VMEM((pool.shape[1], picks.shape[0]), pool.dtype),
            pltpu.SemaphoreType.DMA((rows // block,)),
        ]
    outs = pl.pallas_call(
        functools.partial(sum_kernel, axis, n, count, plan),
        out_shape=shapes,
        in_specs=in_specs,
        out_specs=[vmem] * len(shapes),
        scratch_shapes=scratch,
        compiler_params=pltpu.CompilerParams(
            collective_id=collective_id, has_side_effects=True,
            vmem_limit_bytes=48 * 1024 * 1024,
        ),
        name=f"sum_{axis}_{collective_id}",
    )(*operands)
    return [o.reshape(a.shape) for o, a in zip(outs, arrays)] + list(outs[count:])


def inverse_factor(gram):
    size = gram.shape[0]
    rows = lax.broadcasted_iota(jnp.int32, (size, size), 0)
    columns = lax.broadcasted_iota(jnp.int32, (size, size), 1)
    left = gram
    right = jnp.where(rows == columns, 1.0, 0.0).astype(jnp.float32)
    for k in range(size):
        scale = 1.0 / jnp.sqrt(left[k:k + 1, k:k + 1])
        column = jnp.where(rows[:, :1] > k, left[:, k:k + 1] * scale, 0.0)
        left_row = left[k:k + 1, :] * scale
        right_row = right[k:k + 1, :] * scale
        left = left - column * left_row
        right = jnp.where(rows == k, right_row, right - column * right_row)
    return right


def exact_product(left, right):
    return jnp.dot(
        left, right, precision=lax.Precision.HIGHEST, preferred_element_type=jnp.float32
    )


def normalise_kernel(gram_ref, stepped_ref, *refs):
    inverse = inverse_factor(gram_ref[...])
    if len(refs) == 1:
        refs[0][...] = exact_product(inverse, stepped_ref[...])
        return
    raw_ref, loadings_ref, scores_ref = refs
    scores_ref[...] = exact_product(inverse, raw_ref[...].astype(jnp.float32)).astype(
        scores_ref.dtype
    )
    loadings_ref[...] = exact_product(inverse, stepped_ref[...])


def normalise(gram, stepped, raw=None):
    shapes = [jax.ShapeDtypeStruct(stepped.shape, jnp.float32)]
    operands = [gram, stepped]
    if raw is not None:
        shapes.append(jax.ShapeDtypeStruct(raw.shape, jnp.bfloat16))
        operands.append(raw)
    return pl.pallas_call(
        normalise_kernel,
        out_shape=shapes,
        in_specs=[pl.BlockSpec(memory_space=pltpu.VMEM)] * len(operands),
        out_specs=[pl.BlockSpec(memory_space=pltpu.VMEM)] * len(shapes),
        name="normalise",
    )(*operands)


def select(pool, picks, start):
    ids = jnp.arange(pool.shape[1], dtype=jnp.int32)
    hot = (ids[:, None] == picks[None, :]).astype(pool.dtype)
    return jnp.dot(pool[start:], hot, preferred_element_type=jnp.float32).astype(pool.dtype)


def stacked(x):
    high = x.astype(jnp.bfloat16)
    rest = (x - high.astype(jnp.float32)).astype(jnp.bfloat16)
    return jnp.concatenate([high, rest], axis=0)


def folded(x):
    size = x.shape[0] // 2
    return x[:size] + x[size:]


def whitening(gram):
    size = gram.shape[0]
    rows = lax.broadcasted_iota(jnp.int32, (size, 2 * size), 0)
    columns = lax.broadcasted_iota(jnp.int32, (size, 2 * size), 1)
    state = jnp.concatenate([gram, jnp.zeros_like(gram)], axis=1)
    state = jnp.where(columns == rows + size, 1.0, state)
    for k in range(size):
        scale = lax.rsqrt(state[k:k + 1, k:k + 1])
        column = jnp.where(rows[:, :1] > k, state[:, k:k + 1] * scale, 0.0)
        row = state[k:k + 1, :] * scale
        state = jnp.where(rows == k, row, state - column * row)
    return state[:, size:]


def fused_kernel(
    genes, cells, steps, pool_hbm, picks_ref, init_ref, out_ref,
    pool, pool_t, hot, chosen, sums, mean, stepped, loadings, both, grams, scores, part, landed,
    low, spread, ahead, landed_core, mine, landed_pair, total,
    loaded, sums_send, sums_recv, gram_send, gram_recv, part_send, part_recv, low_send, low_recv,
    core_send, core_recv, pair_send, pair_recv, total_send, total_recv,
):
    me, group = lax.axis_index("gene"), lax.axis_index("cell")
    comps, local = stepped.shape
    local_pool, batch = hot.shape
    width = batch // genes
    block = 256
    half = local // 2
    pieces = half // block
    side = lax.rem(group, 2)
    other_side = 1 - side
    partner = group + 1 - 2 * side
    across = lax.rem(group + 2, cells)
    share = 1.0 / (batch * cells)
    peers = [lax.rem(me + k, genes) for k in range(genes)]
    sources = [lax.rem(me + genes - k, genes) for k in range(genes)]
    barrier = pltpu.get_barrier_semaphore()
    for k in range(1, genes):
        pl.semaphore_signal(barrier, inc=1, device_id={"gene": peers[k]}, device_id_type=MESH)
    for k in range(1, cells):
        pl.semaphore_signal(
            barrier, inc=1, device_id={"cell": lax.rem(group + k, cells)}, device_id_type=MESH
        )

    def load(b):
        rows = pl.ds(pl.multiple_of(b * block, block), block)
        return pltpu.make_async_copy(pool_hbm.at[rows], pool.at[rows], loaded.at[b])

    for b in range(local // block):
        load(b).start()

    def remote(src, dst, send, recv, where):
        return pltpu.make_async_remote_copy(
            src_ref=src, dst_ref=dst, send_sem=send, recv_sem=recv,
            device_id=where, device_id_type=MESH,
        )

    def span(i, size):
        return pl.ds(pl.multiple_of(i * size, 128), size)

    chosen[...] = jnp.zeros_like(chosen)

    for s in range(steps):
        ids = picks_ref[s:s + 1, :] - group * local_pool
        upper = lax.broadcasted_iota(jnp.int32, (local_pool // 128, batch), 0)
        lower = lax.broadcasted_iota(jnp.int32, (128, batch), 0)
        upper = jnp.where(upper == lax.shift_right_logical(ids, 7), 1.0, 0.0).astype(jnp.bfloat16)
        lower = jnp.where(lower == (ids & 127), 1.0, 0.0).astype(jnp.bfloat16)
        counts = transposed_product(upper, lower)
        for h in range(local_pool // 128):
            chosen[s:s + 1, h * 128:(h + 1) * 128] = counts[h:h + 1, :]

    def mark(s):
        ids = picks_ref[pl.ds(s, 1), :] - group * local_pool
        depth = 256

        def piece(i, carry):
            numbers = lax.broadcasted_iota(jnp.int32, (depth, batch), 0) + i * depth
            hot[span(i, depth), :] = jnp.where(numbers == ids, 1.0, 0.0).astype(hot.dtype)
            return carry

        lax.fori_loop(0, local_pool // depth, piece, 0)

    def turn(b, carry):
        load(b).wait()
        rows = span(b, block)
        unit = jnp.where(
            lax.broadcasted_iota(jnp.int32, (block, block), 0)
            == lax.broadcasted_iota(jnp.int32, (block, block), 1), 1.0, 0.0,
        ).astype(jnp.bfloat16)

        def piece(j, inner):
            pool_t[span(j, block), rows] = transposed_product(
                unit, pool[rows, span(j, block)]
            ).astype(pool_t.dtype)
            return inner

        lax.fori_loop(0, local_pool // block, piece, 0)
        sums[group, :, rows] = jnp.dot(
            chosen[...].astype(jnp.bfloat16), pool_t[:, rows], preferred_element_type=jnp.float32
        )
        return carry

    lax.fori_loop(0, local // block, turn, 0)
    pl.semaphore_wait(barrier, genes + cells - 2)
    sums_out = [
        remote(
            sums.at[group], sums.at[group], sums_send.at[k - 1], sums_recv.at[k - 1],
            {"cell": lax.rem(group + k, cells)},
        )
        for k in range(1, cells)
    ]
    for copy in sums_out:
        copy.start()
    mark(0)
    stepped[...] = init_ref[...]
    for copy in sums_out:
        copy.wait()
    whole = sums[0]
    for k in range(1, cells):
        whole = whole + sums[k]
    mean[...] = whole * share

    def gram_copies():
        return [
            remote(
                grams.at[me], grams.at[me], gram_send.at[k - 1], gram_recv.at[k - 1],
                {"gene": peers[k]},
            )
            for k in range(1, genes)
        ]

    def start_gram():
        both[...] = stacked(stepped[...])
        product = folded(transposed_product(both[...], both[...]))
        grams[me] = product[:, :comps] + product[:, comps:]
        for copy in gram_copies():
            copy.start()

    def finish_gram():
        for copy in gram_copies():
            copy.wait_recv()
        gram = grams[0]
        for k in range(1, genes):
            gram = gram + grams[k]
        return whitening(gram)

    def doubled(inverse):
        pair = stacked(inverse)
        return jnp.concatenate([pair, pair], axis=1)

    def step(s, carry):
        start_gram()
        mean_row = mean[pl.ds(s, 1), :]
        high = both[:comps, :]
        shift = jnp.sum(high.astype(jnp.float32) * mean_row, axis=1, keepdims=True)
        wide = 512

        def score(j, inner):
            columns = span(j, wide)
            product = jnp.dot(high, pool[:, columns], preferred_element_type=jnp.float32)
            scores[:, columns] = (product - shift).astype(scores.dtype)
            return inner

        lax.fori_loop(0, local_pool // wide, score, 0)
        outward = [
            remote(
                part.at[peers[k]], landed.at[me], part_send.at[k - 1], part_recv.at[k - 1],
                {"gene": peers[k]},
            )
            for k in range(1, genes)
        ]

        def narrow(j, inner):
            picked = jnp.dot(
                scores[...], hot[:, span(j, 2 * width)], preferred_element_type=jnp.float32
            ).astype(part.dtype)
            part[2 * j] = picked[:, :width]
            part[2 * j + 1] = picked[:, width:]
            return inner

        lax.fori_loop(0, genes // 2, narrow, 0)
        for copy in outward:
            copy.start()
        inverse = finish_gram()
        unit = jnp.where(
            lax.broadcasted_iota(jnp.int32, (comps, comps), 0)
            == lax.broadcasted_iota(jnp.int32, (comps, comps), 1), 1.0, 0.0,
        )
        factor = doubled(jnp.where(s == 0, unit, inverse))

        def apply(j, inner):
            columns = span(j, wide)
            loadings[:, columns] = folded(
                jnp.dot(factor, both[:, columns], preferred_element_type=jnp.float32)
            )
            return inner

        lax.fori_loop(0, local // wide, apply, 0)
        for copy in outward:
            copy.wait_recv()
        landed[me] = part[me]
        raw = landed[0].astype(jnp.float32)
        for k in range(1, genes):
            raw = raw + landed[k].astype(jnp.float32)
        own = span(me, width)
        low[:, own] = folded(
            jnp.dot(factor, stacked(raw), preferred_element_type=jnp.float32)
        ).astype(low.dtype)
        shared = [
            remote(
                low.at[:, own], low.at[:, own], low_send.at[k - 1], low_recv.at[k - 1],
                {"gene": peers[k]},
            )
            for k in range(1, genes)
        ]
        for copy in shared:
            copy.start()
        for copy in shared:
            copy.wait_recv()
        scores_low = low[...]
        row_totals = jnp.sum(scores_low.astype(jnp.float32), axis=1, keepdims=True)

        def widen(j, inner):
            rows = span(j, wide)
            spread[:, rows] = transposed_product(scores_low, hot[rows, :]).astype(spread.dtype)
            return inner

        lax.fori_loop(0, local_pool // wide, widen, 0)

        def partial(columns):
            raw_update = jnp.dot(
                spread[...], pool_t[:, columns], preferred_element_type=jnp.float32
            )
            return (raw_update - row_totals * mean[pl.ds(s, 1), columns]) * share

        def core_copy(j):
            columns = span(j, block)
            return remote(
                ahead.at[:, columns], landed_core.at[:, columns], core_send.at[j], core_recv.at[j],
                {"cell": partner},
            )

        slot = lax.rem(s, 2)

        def pair_copy(j):
            columns = span(j, block)
            return remote(
                mine.at[:, columns], landed_pair.at[slot, :, columns], pair_send.at[j],
                pair_recv.at[slot, j], {"cell": across},
            )

        def total_copy(j, which):
            columns = span(j, block)
            return remote(
                total.at[which, :, columns], total.at[which, :, columns], total_send.at[j],
                total_recv.at[j], {"cell": partner},
            )

        def give(j, inner):
            ahead[:, span(j, block)] = partial(
                pl.ds(pl.multiple_of(other_side * half + j * block, 128), block)
            ).astype(ahead.dtype)
            core_copy(j).start()
            return inner

        lax.fori_loop(0, pieces, give, 0)

        def take(j, inner):
            value = partial(pl.ds(pl.multiple_of(side * half + j * block, 128), block))
            core_copy(j).wait_recv()
            columns = span(j, block)
            mine[:, columns] = (
                value + landed_core[:, columns].astype(jnp.float32)
            ).astype(mine.dtype)
            pair_copy(j).start()
            return inner

        lax.fori_loop(0, pieces, take, 0)
        mark(jnp.minimum(s + 1, steps - 1))

        def join(j, inner):
            pair_copy(j).wait_recv()
            columns = span(j, block)
            value = mine[:, columns].astype(jnp.float32) + landed_pair[slot, :, columns].astype(
                jnp.float32
            )
            total[side, :, columns] = value
            total_copy(j, side).start()
            place = pl.ds(pl.multiple_of(side * half + j * block, 128), block)
            stepped[:, place] = loadings[:, place] + step_rate * value
            return inner

        lax.fori_loop(0, pieces, join, 0)

        def close(j, inner):
            total_copy(j, other_side).wait_recv()
            place = pl.ds(pl.multiple_of(other_side * half + j * block, 128), block)
            stepped[:, place] = (
                loadings[:, place] + step_rate * total[other_side, :, span(j, block)]
            )
            return inner

        lax.fori_loop(0, pieces, close, 0)

        def drain(j, inner):
            core_copy(j).wait_send()
            pair_copy(j).wait_send()
            total_copy(j, side).wait_send()
            return inner

        lax.fori_loop(0, pieces, drain, 0)
        for copy in gram_copies() + outward + shared:
            copy.wait_send()
        return carry

    lax.fori_loop(0, steps, step, 0)
    start_gram()
    factor = doubled(finish_gram() * math.sqrt(local * genes))

    def finish(j, carry):
        columns = span(j, 512)
        out_ref[:, columns] = folded(
            jnp.dot(factor, both[:, columns], preferred_element_type=jnp.float32)
        )
        return carry

    lax.fori_loop(0, local // 512, finish, 0)
    for copy in gram_copies():
        copy.wait_send()


def fits(genes, cells, pool_counts, cell_picks, loadings_init):
    batch = cell_picks.shape[1]
    return (
        cells == 4 and genes % 2 == 0 and batch == 128 * genes and cell_picks.shape[0] <= 8
        and pool_counts.shape[0] % 512 == 0 and pool_counts.shape[1] % 512 == 0
    )


def fused(genes, cells, pool_counts, cell_picks, loadings_init):
    local, local_pool = pool_counts.shape
    steps, batch = cell_picks.shape
    comps = loadings_init.shape[0]
    width = batch // genes
    half = local // 2
    pieces = half // 256
    low, full = jnp.bfloat16, jnp.float32
    vmem = pl.BlockSpec(memory_space=pltpu.VMEM)
    dma = pltpu.SemaphoreType.DMA
    return pl.pallas_call(
        functools.partial(fused_kernel, genes, cells, steps),
        out_shape=jax.ShapeDtypeStruct(loadings_init.shape, full),
        in_specs=[pl.BlockSpec(memory_space=pl.ANY), vmem, vmem],
        out_specs=vmem,
        scratch_shapes=[
            pltpu.VMEM((local, local_pool), low),
            pltpu.VMEM((local_pool, local), low),
            pltpu.VMEM((local_pool, batch), low),
            pltpu.VMEM((8, local_pool), full),
            pltpu.VMEM((cells, 8, local), full),
            pltpu.VMEM((8, local), full),
            pltpu.VMEM((comps, local), full),
            pltpu.VMEM((comps, local), full),
            pltpu.VMEM((2 * comps, local), low),
            pltpu.VMEM((genes, comps, comps), full),
            pltpu.VMEM((comps, local_pool), low),
            pltpu.VMEM((genes, comps, width), low),
            pltpu.VMEM((genes, comps, width), low),
            pltpu.VMEM((comps, batch), low),
            pltpu.VMEM((comps, local_pool), low),
            pltpu.VMEM((comps, half), low),
            pltpu.VMEM((comps, half), low),
            pltpu.VMEM((comps, half), low),
            pltpu.VMEM((2, comps, half), low),
            pltpu.VMEM((2, comps, half), full),
            dma((local // 256,)),
            dma((cells - 1,)), dma((cells - 1,)),
            dma((genes - 1,)), dma((genes - 1,)),
            dma((genes - 1,)), dma((genes - 1,)),
            dma((genes - 1,)), dma((genes - 1,)),
            dma((pieces,)), dma((pieces,)),
            dma((pieces,)), dma((2, pieces)),
            dma((pieces,)), dma((pieces,)),
        ],
        compiler_params=pltpu.CompilerParams(
            collective_id=8, has_side_effects=True, vmem_limit_bytes=66_000_000,
        ),
        name="fused_steps",
    )(pool_counts, cell_picks, loadings_init)


def shards(genes, cells, pool_counts, cell_picks, loadings_init):
    if fits(genes, cells, pool_counts, cell_picks, loadings_init):
        return fused(genes, cells, pool_counts, cell_picks, loadings_init)
    stepped = loadings_init
    local_pool = pool_counts.shape[1]
    group = lax.axis_index("cell")
    batch_total = cell_picks.shape[1] * cells
    local_genes = stepped.shape[1]
    gene_total = local_genes * genes
    picks = cell_picks - group * local_pool
    ids = jnp.arange(local_pool, dtype=jnp.int32)
    chosen = jnp.any(picks[:, :, None] == ids[None, None, :], axis=1).astype(jnp.bfloat16)
    sums = transposed_product(chosen, pool_counts)
    sums = jnp.pad(sums, ((0, -STEPS % cells), (0, 0)))
    split = local_genes // 2
    totals, upper = sum_over("cell", cells, 1, [sums], (pool_counts, picks[0], 0, split))
    lower = select(pool_counts, picks[0], split)
    means = totals / batch_total
    for s in range(STEPS):
        last = s == STEPS - 1
        mean = means[s]
        low = stepped.astype(jnp.bfloat16)
        product = jnp.dot(low[:, :split], upper, preferred_element_type=jnp.float32)
        product += jnp.dot(low[:, split:], lower, preferred_element_type=jnp.float32)
        shift = jnp.dot(low.astype(jnp.float32), mean, precision=lax.Precision.HIGHEST)
        part = (product - shift[:, None]).astype(jnp.bfloat16)
        ahead = None if last else (pool_counts, picks[s + 1], 0, split)
        if s == 0:
            scores_low, *next_upper = sum_over("gene", genes, 2, [part], ahead)
            loadings = stepped
        else:
            gram_part = jnp.dot(stepped, stepped.T, precision=lax.Precision.HIGHEST)
            raw, gram, *next_upper = sum_over(
                "gene", genes, 6 if last else 3, [part, gram_part], ahead
            )
            loadings, scores_low = normalise(gram, stepped, raw)
        raw_update = jnp.concatenate(
            [transposed_product(scores_low, upper), transposed_product(scores_low, lower)], axis=1
        )
        row_totals = jnp.sum(scores_low, axis=1, dtype=jnp.float32)
        local = (raw_update - row_totals[:, None] * mean[None, :]) / batch_total
        ahead = None if last else (pool_counts, picks[s + 1], split, local_genes - split)
        update, *next_lower = sum_over(
            "cell", cells, 7 if last else 4, [local.astype(jnp.bfloat16)], ahead
        )
        if not last:
            upper, lower = next_upper[0], next_lower[0]
        stepped = loadings + step_rate * update.astype(jnp.float32)
    gram_part = jnp.dot(stepped, stepped.T, precision=lax.Precision.HIGHEST)
    (gram,) = sum_over("gene", genes, 5, [gram_part])
    (loadings,) = normalise(gram, stepped)
    return loadings * math.sqrt(gene_total)


def solution(mesh):
    placed = (P("gene", "cell"), P(None, "cell"), P(None, "gene"))
    return jax.shard_map(
        functools.partial(shards, mesh.shape["gene"], mesh.shape["cell"]),
        mesh=mesh, in_specs=placed, out_specs=P(None, "gene"), check_vma=False,
    )
```

```python
import functools
import math

import jax
import jax.numpy as jnp
from jax import lax
from jax.experimental import pallas as pl
from jax.experimental.pallas import tpu as pltpu
from jax.sharding import PartitionSpec as P

STEPS = 7
MESH = pl.DeviceIdType.MESH

step_rate = 1.0


def transposed_product(left, right):
    return lax.dot_general(
        left, right, (((1,), (1,)), ((), ())), preferred_element_type=jnp.float32
    )


def sum_kernel(axis, n, arrays, gather, *refs):
    inputs = refs[:arrays]
    refs = refs[arrays:]
    if gather:
        pool_ref, picks_ref = refs[:2]
        refs = refs[2:]
    outputs = refs[:arrays]
    refs = refs[arrays:]
    if gather:
        tile_ref = refs[0]
        refs = refs[1:]
    landed, reduced, whole = (refs[i * arrays:(i + 1) * arrays] for i in range(3))
    sends, arrivals, sends_back, arrivals_back = refs[3 * arrays:3 * arrays + 4]
    me = lax.axis_index(axis)
    barrier = pltpu.get_barrier_semaphore()
    peers = [lax.rem(me + k, n) for k in range(n)]
    for k in range(1, n):
        pl.semaphore_signal(barrier, inc=1, device_id={axis: peers[k]}, device_id_type=MESH)
    blocks = 0
    if gather:
        held, hot, loaded = refs[3 * arrays + 4:]
        start, block, blocks = gather
        loads = []
        for b in range(blocks):
            load = pltpu.make_async_copy(
                pool_ref.at[pl.ds(start + b * block, block)],
                held.at[pl.ds(b * block, block)],
                loaded.at[b],
            )
            load.start()
            loads.append(load)

    def select_columns(b):
        loads[b].wait()
        rows = pl.ds(b * block, block)
        width = min(512, hot.shape[1])

        def piece(j, carry):
            columns = pl.ds(pl.multiple_of(j * width, width), width)
            tile_ref[rows, columns] = jnp.dot(
                held[rows, :], hot[:, columns], preferred_element_type=jnp.float32
            ).astype(tile_ref.dtype)
            return carry

        lax.fori_loop(0, hot.shape[1] // width, piece, 0)

    pl.semaphore_wait(barrier, n - 1)
    copies = []
    for a in range(arrays):
        for k in range(1, n):
            copy = pltpu.make_async_remote_copy(
                src_ref=inputs[a].at[peers[k]],
                dst_ref=landed[a].at[k - 1],
                send_sem=sends.at[a, k - 1],
                recv_sem=arrivals.at[a, k - 1],
                device_id={axis: peers[k]},
                device_id_type=MESH,
            )
            copy.start()
            copies.append(copy)
    if gather:
        depth = 256

        def mark(i, carry):
            ids = lax.broadcasted_iota(jnp.int32, (depth, hot.shape[1]), 0) + i * depth
            hot[pl.ds(pl.multiple_of(i * depth, depth), depth), :] = jnp.where(
                ids == picks_ref[...], 1.0, 0.0
            ).astype(hot.dtype)
            return carry

        lax.fori_loop(0, hot.shape[0] // depth, mark, 0)
    early = blocks // 2
    for b in range(early):
        select_columns(b)
    for copy in copies:
        copy.wait_recv()
    backs = []
    for a in range(arrays):
        total = inputs[a][me].astype(jnp.float32)
        for k in range(1, n):
            total = total + landed[a][k - 1].astype(jnp.float32)
        reduced[a][...] = total.astype(reduced[a].dtype)
        for k in range(1, n):
            copy = pltpu.make_async_remote_copy(
                src_ref=reduced[a],
                dst_ref=whole[a].at[me],
                send_sem=sends_back.at[a, k - 1],
                recv_sem=arrivals_back.at[a, k - 1],
                device_id={axis: peers[k]},
                device_id_type=MESH,
            )
            copy.start()
            backs.append(copy)
        outputs[a][me] = reduced[a][...]
    for b in range(early, blocks):
        select_columns(b)
    for copy in copies:
        copy.wait_send()
    for copy in backs:
        copy.wait()
    for a in range(arrays):
        for k in range(1, n):
            outputs[a][peers[k]] = whole[a][peers[k]]


def sum_over(axis, n, collective_id, arrays, gather=None):
    cut = [a.reshape(n, a.shape[0] // n, a.shape[1]) for a in arrays]
    count = len(cut)
    vmem = pl.BlockSpec(memory_space=pltpu.VMEM)
    operands, in_specs = list(cut), [vmem] * count
    shapes = [jax.ShapeDtypeStruct(a.shape, a.dtype) for a in cut]
    scratch = [pltpu.VMEM((n - 1,) + a.shape[1:], a.dtype) for a in cut]
    scratch += [pltpu.VMEM(a.shape[1:], a.dtype) for a in cut]
    scratch += [pltpu.VMEM(a.shape, a.dtype) for a in cut]
    scratch += [pltpu.SemaphoreType.DMA((count, n - 1))] * 4
    plan = None
    if gather is not None:
        pool, picks, start, rows = gather
        block = 256 if rows % 256 == 0 else rows
        plan = (start, block, rows // block)
        operands += [pool, picks[None, :]]
        in_specs += [pl.BlockSpec(memory_space=pl.ANY), vmem]
        shapes.append(jax.ShapeDtypeStruct((rows, picks.shape[0]), pool.dtype))
        scratch += [
            pltpu.VMEM((rows, pool.shape[1]), pool.dtype),
            pltpu.VMEM((pool.shape[1], picks.shape[0]), pool.dtype),
            pltpu.SemaphoreType.DMA((rows // block,)),
        ]
    outs = pl.pallas_call(
        functools.partial(sum_kernel, axis, n, count, plan),
        out_shape=shapes,
        in_specs=in_specs,
        out_specs=[vmem] * len(shapes),
        scratch_shapes=scratch,
        compiler_params=pltpu.CompilerParams(
            collective_id=collective_id, has_side_effects=True,
            vmem_limit_bytes=48 * 1024 * 1024,
        ),
        name=f"sum_{axis}_{collective_id}",
    )(*operands)
    return [o.reshape(a.shape) for o, a in zip(outs, arrays)] + list(outs[count:])


def inverse_factor(gram):
    size = gram.shape[0]
    rows = lax.broadcasted_iota(jnp.int32, (size, size), 0)
    columns = lax.broadcasted_iota(jnp.int32, (size, size), 1)
    left = gram
    right = jnp.where(rows == columns, 1.0, 0.0).astype(jnp.float32)
    for k in range(size):
        scale = 1.0 / jnp.sqrt(left[k:k + 1, k:k + 1])
        column = jnp.where(rows[:, :1] > k, left[:, k:k + 1] * scale, 0.0)
        left_row = left[k:k + 1, :] * scale
        right_row = right[k:k + 1, :] * scale
        left = left - column * left_row
        right = jnp.where(rows == k, right_row, right - column * right_row)
    return right


def exact_product(left, right):
    return jnp.dot(
        left, right, precision=lax.Precision.HIGHEST, preferred_element_type=jnp.float32
    )


def normalise_kernel(gram_ref, stepped_ref, *refs):
    inverse = inverse_factor(gram_ref[...])
    if len(refs) == 1:
        refs[0][...] = exact_product(inverse, stepped_ref[...])
        return
    raw_ref, loadings_ref, scores_ref = refs
    scores_ref[...] = exact_product(inverse, raw_ref[...].astype(jnp.float32)).astype(
        scores_ref.dtype
    )
    loadings_ref[...] = exact_product(inverse, stepped_ref[...])


def normalise(gram, stepped, raw=None):
    shapes = [jax.ShapeDtypeStruct(stepped.shape, jnp.float32)]
    operands = [gram, stepped]
    if raw is not None:
        shapes.append(jax.ShapeDtypeStruct(raw.shape, jnp.bfloat16))
        operands.append(raw)
    return pl.pallas_call(
        normalise_kernel,
        out_shape=shapes,
        in_specs=[pl.BlockSpec(memory_space=pltpu.VMEM)] * len(operands),
        out_specs=[pl.BlockSpec(memory_space=pltpu.VMEM)] * len(shapes),
        name="normalise",
    )(*operands)


def select(pool, picks, start):
    ids = jnp.arange(pool.shape[1], dtype=jnp.int32)
    hot = (ids[:, None] == picks[None, :]).astype(pool.dtype)
    return jnp.dot(pool[start:], hot, preferred_element_type=jnp.float32).astype(pool.dtype)


def stacked(x):
    high = x.astype(jnp.bfloat16)
    rest = (x - high.astype(jnp.float32)).astype(jnp.bfloat16)
    return jnp.concatenate([high, rest], axis=0)


def folded(x):
    size = x.shape[0] // 2
    return x[:size] + x[size:]


def whitening(gram):
    size, panel = gram.shape[0], 8
    wide = 2 * size
    rows = lax.broadcasted_iota(jnp.int32, (size, wide), 0)
    columns = lax.broadcasted_iota(jnp.int32, (size, wide), 1)
    state = jnp.concatenate([gram, jnp.zeros_like(gram)], axis=1)
    rest = jnp.where(columns == rows + size, 1.0, state)
    done = []
    for first in range(0, size, panel):
        height = size - first
        local = rows[:height]
        bands = [
            jnp.broadcast_to(rest[:, first + j:first + j + 1], (height, wide))
            for j in range(panel)
        ]
        top = rest[:panel]
        below = rest[panel:]
        for j in range(panel):
            scale = lax.rsqrt(bands[j][j:j + 1, :])
            column = jnp.where(local > j, bands[j] * scale, 0.0)
            for i in range(j + 1, panel):
                bands[i] = bands[i] - column * (bands[i][j:j + 1, :] * scale)
            row = top[j:j + 1, :] * scale
            top = jnp.where(local[:panel] == j, row, top - column[:panel] * row)
            if height > panel:
                below = below - column[panel:] * row
        done.append(top)
        rest = below
    return jnp.concatenate(done, axis=0)[:, size:]


def fused_kernel(
    genes, cells, steps, pool_hbm, picks_ref, lists_ref, init_hbm, out_hbm,
    pool, pool_t, hot, hot_t, marks, chosen, sums, mean, loadings, both, gram_part, shifts, gathered,
    gram_out, gram_in, grams, scores, part, landed, low, ahead, kept, landed_core, mine, landed_pair, total,
    loaded, moved, sums_send, sums_recv, gram_send, gram_recv, share_send, share_recv, part_send, part_recv,
    low_send, low_recv, core_send, core_recv, pair_send, pair_recv, total_send, total_recv,
):
    me, group = lax.axis_index("gene"), lax.axis_index("cell")
    comps, local = loadings.shape
    local_pool, batch = hot.shape
    width = batch // genes
    block, wide = 256, 512
    half = local // 2
    pieces = half // block
    side = lax.rem(group, 2)
    other_side = 1 - side
    partner = group + 1 - 2 * side
    across = lax.rem(group + 2, cells)
    share = 1.0 / (batch * cells)
    peers = [lax.rem(me + k, genes) for k in range(genes)]
    barrier = pltpu.get_barrier_semaphore()
    for k in range(1, genes):
        pl.semaphore_signal(barrier, inc=1, device_id={"gene": peers[k]}, device_id_type=MESH)
    for k in range(1, cells):
        pl.semaphore_signal(
            barrier, inc=1, device_id={"cell": lax.rem(group + k, cells)}, device_id_type=MESH
        )

    def span(i, size):
        return pl.ds(pl.multiple_of(i * size, 128), size)

    def load(b):
        return pltpu.make_async_copy(
            pool_hbm.at[span(b, block)], pool.at[span(b, block)], loaded.at[b]
        )

    take_init = pltpu.make_async_copy(init_hbm, loadings, moved.at[0])
    take_init.start()
    for b in range(local // block):
        load(b).start()

    def remote(src, dst, send, recv, where):
        return pltpu.make_async_remote_copy(
            src_ref=src, dst_ref=dst, send_sem=send, recv_sem=recv,
            device_id=where, device_id_type=MESH,
        )

    def equal_mask(size):
        return (
            lax.broadcasted_iota(jnp.int32, (size, size), 0)
            == lax.broadcasted_iota(jnp.int32, (size, size), 1)
        )

    chosen[...] = jnp.zeros_like(chosen)
    for s in range(steps):
        ids = picks_ref[s:s + 1, :] - group * local_pool
        upper = lax.broadcasted_iota(jnp.int32, (local_pool // 128, batch), 0)
        lower = lax.broadcasted_iota(jnp.int32, (128, batch), 0)
        upper = jnp.where(upper == lax.shift_right_logical(ids, 7), 1.0, 0.0).astype(jnp.bfloat16)
        lower = jnp.where(lower == (ids & 127), 1.0, 0.0).astype(jnp.bfloat16)
        counts = transposed_product(upper, lower)
        for h in range(local_pool // 128):
            chosen[s:s + 1, h * 128:(h + 1) * 128] = counts[h:h + 1, :]

    def mark(s):
        ids = picks_ref[pl.ds(s, 1), :] - group * local_pool
        numbers = lax.broadcasted_iota(jnp.int32, (128, batch), 0)
        marks[...] = jnp.where(numbers == (ids & 127), 1.0, 0.0).astype(marks.dtype)
        tiles = jnp.broadcast_to(
            lax.shift_right_logical(ids, 7).astype(jnp.float32), (16, batch)
        ).astype(jnp.bfloat16)
        for i in range(local_pool // 128):
            here = tiles == jnp.bfloat16(i)
            for k in range(8):
                rows = slice(k * 16, (k + 1) * 16)
                hot[i * 128 + k * 16:i * 128 + (k + 1) * 16, :] = jnp.where(
                    here, marks[rows, :], jnp.bfloat16(0)
                )

    def mark_turned(s):
        ids = lists_ref[s] - group * local_pool
        upper = lax.shift_right_logical(ids, 7).astype(jnp.float32).T
        lower = (ids & 127).astype(jnp.float32).T
        lanes = lax.broadcasted_iota(jnp.int32, (128, 128), 1).astype(jnp.float32)
        for h in range(batch // 128):
            found = jnp.where(
                lanes == jnp.broadcast_to(lower[:, h:h + 1], (128, 128)), 1.0, 0.0
            ).astype(jnp.bfloat16)
            tiles = jnp.broadcast_to(upper[:, h:h + 1], (128, 128)).astype(jnp.bfloat16)
            for i in range(local_pool // 128):
                hot_t[h * 128:(h + 1) * 128, i * 128:(i + 1) * 128] = jnp.where(
                    tiles == jnp.bfloat16(i), found, jnp.bfloat16(0)
                )

    def absorb(*arrived, fresh=False):
        highs = []
        product = 0.0 if fresh else gram_part[...]
        for place, value in arrived:
            pair = stacked(value)
            both[:, place] = pair
            highs.append(pair[:comps])
            product = product + transposed_product(pair, pair)
        gram_part[...] = product
        for j in range(local_pool // wide):
            columns = slice(j * wide, (j + 1) * wide)
            product = sum(
                jnp.dot(high, pool[place, columns], preferred_element_type=jnp.float32)
                for high, (place, _) in zip(highs, arrived)
            )
            gathered[:, columns] = product if fresh else gathered[:, columns] + product

    def note_shift(place, s):
        value = both[:comps, place].astype(jnp.float32) * mean[pl.ds(s, 1), place]
        shifts[...] = shifts[...] + value[:, :128] + value[:, 128:]

    gram_part[...] = jnp.zeros_like(gram_part)
    shifts[...] = jnp.zeros_like(shifts)
    gathered[...] = jnp.zeros_like(gathered)
    take_init.wait()
    chosen_low = chosen[...].astype(jnp.bfloat16)

    def read(b, carry):
        load(b).wait()
        rows = span(b, block)
        sums[group, :, rows] = transposed_product(chosen_low, pool[rows, :])
        absorb((rows, loadings[:, rows]))
        return carry

    lax.fori_loop(0, local // block, read, 0)
    pl.semaphore_wait(barrier, genes + cells - 2)
    sums_out = [
        remote(
            sums.at[group], sums.at[group], sums_send.at[k - 1], sums_recv.at[k - 1],
            {"cell": lax.rem(group + k, cells)},
        )
        for k in range(1, cells)
    ]
    for copy in sums_out:
        copy.start()

    def gram_copies():
        return [
            remote(
                gram_out.at[peers[k]], gram_in.at[me], gram_send.at[k - 1], gram_recv.at[k - 1],
                {"gene": peers[k]},
            )
            for k in range(1, genes)
        ]

    def gram_shares():
        return [
            remote(
                grams.at[me], grams.at[me], share_send.at[k - 1], share_recv.at[k - 1],
                {"gene": peers[k]},
            )
            for k in range(1, genes)
        ]

    def start_gram():
        product = folded(gram_part[...])
        product = product[:, :comps] + product[:, comps:]
        packed = jnp.concatenate([product[:comps // 2], product[comps // 2:]], axis=1)
        height = gram_out.shape[1]
        for k in range(genes):
            gram_out[k] = packed[k * height:(k + 1) * height]
        for copy in gram_copies():
            copy.start()

    def share_gram():
        for copy in gram_copies():
            copy.wait_recv()
        gram_in[me] = gram_out[me]
        gram = gram_in[0]
        for k in range(1, genes):
            gram = gram + gram_in[k]
        grams[me] = gram
        for copy in gram_shares():
            copy.start()

    def finish_gram():
        for copy in gram_shares():
            copy.wait_recv()
        gram = jnp.concatenate([grams[k] for k in range(genes)], axis=0)
        return whitening(jnp.concatenate([gram[:, :comps], gram[:, comps:]], axis=0))

    def doubled(inverse):
        pair = stacked(inverse)
        return jnp.concatenate([pair, pair], axis=1)

    unit = jnp.where(equal_mask(block), 1.0, 0.0).astype(jnp.bfloat16)

    def turn(b, carry):
        rows = span(b, block)

        for j in range(local_pool // block):
            cells_here = slice(j * block, (j + 1) * block)
            pool_t[cells_here, rows] = transposed_product(
                unit, pool[rows, cells_here]
            ).astype(pool_t.dtype)
        return carry

    lax.fori_loop(0, local // block, turn, 0)
    mark(0)
    for copy in sums_out:
        copy.wait()
    whole = sums[0]
    for k in range(1, cells):
        whole = whole + sums[k]
    mean[...] = whole * share

    def first_shift(b, carry):
        note_shift(span(b, block), 0)
        return carry

    lax.fori_loop(0, local // block, first_shift, 0)

    def total_copy(j, which):
        columns = span(j, block)
        return remote(
            total.at[which, :, columns], total.at[which, :, columns], total_send.at[j],
            total_recv.at[j], {"cell": partner},
        )

    def part_copy(peer):
        return remote(
            part.at[peer], landed.at[me], part_send.at[peer], part_recv.at[me], {"gene": peer}
        )

    def arrival(source):
        return remote(
            part.at[source], landed.at[source], part_send.at[source], part_recv.at[source],
            {"gene": source},
        )

    def step(s, carry):
        start_gram()
        shift = jnp.sum(shifts[...], axis=1, keepdims=True)
        scores[...] = (gathered[...] - shift).astype(scores.dtype)

        pairs = [lax.rem(j + me // 2 + 1, genes // 2) for j in range(genes // 2)]
        for first in range(0, genes // 2, 2):
            for pair in pairs[first:first + 2]:
                picked = jnp.dot(
                    scores[...], hot[:, span(pair, 2 * width)], preferred_element_type=jnp.float32
                ).astype(part.dtype)
                for k in range(2):
                    part[2 * pair + k] = picked[:, k * width:(k + 1) * width]
            for j in range(first, min(first + 2, genes // 2)):
                if j < genes // 2 - 1:
                    part_copy(2 * pairs[j]).start()
                    part_copy(2 * pairs[j] + 1).start()
                else:
                    part_copy(me + 1 - 2 * lax.rem(me, 2)).start()
        share_gram()
        for k in range(1, genes):
            arrival(peers[k]).wait_recv()
        landed[me] = part[me]
        raw = landed[0].astype(jnp.float32)
        for k in range(1, genes):
            raw = raw + landed[k].astype(jnp.float32)
        own = span(me, width)
        low[:, own] = raw.astype(low.dtype)
        shared = [
            remote(
                low.at[:, own], low.at[:, own], low_send.at[k - 1], low_recv.at[k - 1],
                {"gene": peers[k]},
            )
            for k in range(1, genes)
        ]
        for copy in shared:
            copy.start()

        mark_turned(s)
        inverse = finish_gram()
        pair = stacked(jnp.where(s == 0, jnp.where(equal_mask(comps), 1.0, 0.0), inverse))
        factor = jnp.concatenate([pair, pair], axis=1)
        for j in range(local // wide):
            columns = slice(j * wide, (j + 1) * wide)
            loadings[:, columns] = folded(
                jnp.dot(factor, both[:, columns], preferred_element_type=jnp.float32)
            )
        for copy in gram_copies() + gram_shares():
            copy.wait_send()
        for k in range(1, genes):
            part_copy(peers[k]).wait_send()

        @pl.when(s > 0)
        def _():
            for j in range(pieces):
                total_copy(j, side).wait_send()

        for copy in shared:
            copy.wait_recv()
        scores_low = folded(
            jnp.dot(pair, low[...], preferred_element_type=jnp.float32)
        ).astype(low.dtype)
        row_totals = jnp.sum(scores_low.astype(jnp.float32), axis=1, keepdims=True)

        for j in range(local_pool // wide):
            columns = slice(j * wide, (j + 1) * wide)
            scores[:, columns] = jnp.dot(
                scores_low, hot_t[:, columns], preferred_element_type=jnp.float32
            ).astype(scores.dtype)

        def place_of(which, j):
            return pl.ds(pl.multiple_of(which * half + j * block, 128), block)

        def partial(columns):
            raw_update = jnp.dot(
                scores[...], pool_t[:, columns], preferred_element_type=jnp.float32
            )
            return (raw_update - row_totals * mean[pl.ds(s, 1), columns]) * share

        def core_copy(j):
            columns = span(j, block)
            return remote(
                ahead.at[:, columns], landed_core.at[:, columns], core_send.at[j], core_recv.at[j],
                {"cell": partner},
            )

        slot = lax.rem(s, 2)

        def pair_copy(j):
            columns = span(j, block)
            return remote(
                mine.at[:, columns], landed_pair.at[slot, :, columns], pair_send.at[j],
                pair_recv.at[slot, j], {"cell": across},
            )

        def take(j):
            core_copy(j).wait_recv()
            columns = span(j, block)
            mine[:, columns] = (
                kept[:, columns] + landed_core[:, columns].astype(jnp.float32)
            ).astype(mine.dtype)
            pair_copy(j).start()

        def give(places):
            for j in places:
                ahead[:, span(j, block)] = partial(place_of(other_side, j)).astype(ahead.dtype)

        def keep(places):
            for j in places:
                kept[:, span(j, block)] = partial(place_of(side, j))

        early = min(2, pieces)
        give(range(early))
        for j in range(early):
            core_copy(j).start()
        give(range(early, pieces))
        keep(range(1))
        for j in range(early, pieces):
            core_copy(j).start()
        take(0)
        for first in range(1, pieces, 2):
            together = range(first, min(first + 2, pieces))
            keep(together)
            for j in together:
                take(j)
        later = jnp.minimum(s + 1, steps - 1)
        mark(later)

        def join(j):
            pair_copy(j).wait_recv()
            columns = span(j, block)
            value = mine[:, columns].astype(jnp.float32) + landed_pair[slot, :, columns].astype(
                jnp.float32
            )
            total[side, :, columns] = value
            total_copy(j, side).start()
            place = place_of(side, j)
            return place, loadings[:, place] + step_rate * value

        def close(j):
            total_copy(j, other_side).wait_recv()
            place = place_of(other_side, j)
            return place, loadings[:, place] + step_rate * total[other_side, :, span(j, block)]

        def settle_in(*arrived, fresh=False):
            absorb(*arrived, fresh=fresh)
            if fresh:
                shifts[...] = jnp.zeros_like(shifts)
            for place, _ in arrived:
                note_shift(place, later)

        before = []
        for first in range(0, pieces, 2):
            now = range(first, min(first + 2, pieces))
            settle_in(*[join(j) for j in now], *[close(j) for j in before], fresh=first == 0)
            before = now
        settle_in(*[close(j) for j in before])
        for j in range(pieces):
            core_copy(j).wait_send()
            pair_copy(j).wait_send()
        for copy in shared:
            copy.wait_send()
        return carry

    lax.fori_loop(0, steps, step, 0)
    start_gram()
    share_gram()
    factor = doubled(finish_gram() * math.sqrt(local * genes))

    def give_out(j):
        return pltpu.make_async_copy(
            loadings.at[:, span(j, wide)], out_hbm.at[:, span(j, wide)], moved.at[1 + j]
        )

    def finish(j, carry):
        columns = span(j, wide)
        loadings[:, columns] = folded(
            jnp.dot(factor, both[:, columns], preferred_element_type=jnp.float32)
        )
        give_out(j).start()
        return carry

    lax.fori_loop(0, local // wide, finish, 0)
    for j in range(local // wide):
        give_out(j).wait()
    for copy in gram_copies() + gram_shares():
        copy.wait_send()
    for j in range(pieces):
        total_copy(j, side).wait_send()


def fits(genes, cells, pool_counts, cell_picks, loadings_init):
    batch = cell_picks.shape[1]
    return (
        cells == 4 and genes % 2 == 0 and batch == 128 * genes and cell_picks.shape[0] <= 8
        and pool_counts.shape[0] % 512 == 0 and pool_counts.shape[1] % 1024 == 0
    )


def fused(genes, cells, pool_counts, cell_picks, loadings_init):
    local, local_pool = pool_counts.shape
    steps, batch = cell_picks.shape
    comps = loadings_init.shape[0]
    width = batch // genes
    half = local // 2
    pieces = half // 256
    low, full = jnp.bfloat16, jnp.float32
    vmem, anywhere = pl.BlockSpec(memory_space=pltpu.VMEM), pl.BlockSpec(memory_space=pl.ANY)
    dma = pltpu.SemaphoreType.DMA
    return pl.pallas_call(
        functools.partial(fused_kernel, genes, cells, steps),
        out_shape=jax.ShapeDtypeStruct(loadings_init.shape, full),
        in_specs=[anywhere, vmem, vmem, anywhere],
        out_specs=anywhere,
        scratch_shapes=[
            pltpu.VMEM((local, local_pool), low),
            pltpu.VMEM((local_pool, local), low),
            pltpu.VMEM((local_pool, batch), low),
            pltpu.VMEM((batch, local_pool), low),
            pltpu.VMEM((128, batch), low),
            pltpu.VMEM((8, local_pool), full),
            pltpu.VMEM((cells, 8, local), full),
            pltpu.VMEM((8, local), full),
            pltpu.VMEM((comps, local), full),
            pltpu.VMEM((2 * comps, local), low),
            pltpu.VMEM((2 * comps, 2 * comps), full),
            pltpu.VMEM((comps, 128), full),
            pltpu.VMEM((comps, local_pool), full),
            pltpu.VMEM((genes, comps // 2 // genes, 2 * comps), full),
            pltpu.VMEM((genes, comps // 2 // genes, 2 * comps), full),
            pltpu.VMEM((genes, comps // 2 // genes, 2 * comps), full),
            pltpu.VMEM((comps, local_pool), low),
            pltpu.VMEM((genes, comps, width), low),
            pltpu.VMEM((genes, comps, width), low),
            pltpu.VMEM((comps, batch), low),
            pltpu.VMEM((comps, half), low),
            pltpu.VMEM((comps, half), full),
            pltpu.VMEM((comps, half), low),
            pltpu.VMEM((comps, half), low),
            pltpu.VMEM((2, comps, half), low),
            pltpu.VMEM((2, comps, half), full),
            dma((local // 256,)), dma((1 + local // 512,)),
            dma((cells - 1,)), dma((cells - 1,)),
            dma((genes - 1,)), dma((genes - 1,)),
            dma((genes - 1,)), dma((genes - 1,)),
            dma((genes,)), dma((genes,)),
            dma((genes - 1,)), dma((genes - 1,)),
            dma((pieces,)), dma((pieces,)),
            dma((pieces,)), dma((2, pieces)),
            dma((pieces,)), dma((pieces,)),
        ],
        compiler_params=pltpu.CompilerParams(
            collective_id=8, has_side_effects=True, vmem_limit_bytes=67_000_000,
        ),
        name="fused_steps",
    )(pool_counts, cell_picks, cell_picks.reshape(steps, batch // 128, 128), loadings_init)


def shards(genes, cells, pool_counts, cell_picks, loadings_init):
    if fits(genes, cells, pool_counts, cell_picks, loadings_init):
        return fused(genes, cells, pool_counts, cell_picks, loadings_init)
    stepped = loadings_init
    local_pool = pool_counts.shape[1]
    group = lax.axis_index("cell")
    batch_total = cell_picks.shape[1] * cells
    local_genes = stepped.shape[1]
    gene_total = local_genes * genes
    picks = cell_picks - group * local_pool
    ids = jnp.arange(local_pool, dtype=jnp.int32)
    chosen = jnp.any(picks[:, :, None] == ids[None, None, :], axis=1).astype(jnp.bfloat16)
    sums = transposed_product(chosen, pool_counts)
    sums = jnp.pad(sums, ((0, -STEPS % cells), (0, 0)))
    split = local_genes // 2
    totals, upper = sum_over("cell", cells, 1, [sums], (pool_counts, picks[0], 0, split))
    lower = select(pool_counts, picks[0], split)
    means = totals / batch_total
    for s in range(STEPS):
        last = s == STEPS - 1
        mean = means[s]
        low = stepped.astype(jnp.bfloat16)
        product = jnp.dot(low[:, :split], upper, preferred_element_type=jnp.float32)
        product += jnp.dot(low[:, split:], lower, preferred_element_type=jnp.float32)
        shift = jnp.dot(low.astype(jnp.float32), mean, precision=lax.Precision.HIGHEST)
        part = (product - shift[:, None]).astype(jnp.bfloat16)
        ahead = None if last else (pool_counts, picks[s + 1], 0, split)
        if s == 0:
            scores_low, *next_upper = sum_over("gene", genes, 2, [part], ahead)
            loadings = stepped
        else:
            gram_part = jnp.dot(stepped, stepped.T, precision=lax.Precision.HIGHEST)
            raw, gram, *next_upper = sum_over(
                "gene", genes, 6 if last else 3, [part, gram_part], ahead
            )
            loadings, scores_low = normalise(gram, stepped, raw)
        raw_update = jnp.concatenate(
            [transposed_product(scores_low, upper), transposed_product(scores_low, lower)], axis=1
        )
        row_totals = jnp.sum(scores_low, axis=1, dtype=jnp.float32)
        local = (raw_update - row_totals[:, None] * mean[None, :]) / batch_total
        ahead = None if last else (pool_counts, picks[s + 1], split, local_genes - split)
        update, *next_lower = sum_over(
            "cell", cells, 7 if last else 4, [local.astype(jnp.bfloat16)], ahead
        )
        if not last:
            upper, lower = next_upper[0], next_lower[0]
        stepped = loadings + step_rate * update.astype(jnp.float32)
    gram_part = jnp.dot(stepped, stepped.T, precision=lax.Precision.HIGHEST)
    (gram,) = sum_over("gene", genes, 5, [gram_part])
    (loadings,) = normalise(gram, stepped)
    return loadings * math.sqrt(gene_total)


def solution(mesh):
    placed = (P("gene", "cell"), P(None, "cell"), P(None, "gene"))
    return jax.shard_map(
        functools.partial(shards, mesh.shape["gene"], mesh.shape["cell"]),
        mesh=mesh, in_specs=placed, out_specs=P(None, "gene"), check_vma=False,
    )
```
